32 devices in a mesh: vocab: 8 (over z, x), width: 4 (over y, core).
Axes of the slice: x: 2, y: 2, z: 4, core: 2. Of those that a mesh axis runs over, the one named last changes fastest.
Arguments:
- token_ids: int32 [416], replicated, may hold values from 0 to 4799, as said below
- hidden: bfloat16 [416, 8192], P('vocab', 'width'), may hold values from -6 to 6
- embed_cot: bfloat16 [416, 8192], P('vocab', 'width'), may hold values from -6 to 6
- logit_cot: bfloat16 [416, 4800], P('width', 'vocab'), may hold values from -0.8660254 to 0.8660254
- emb_first: bfloat16 [4800, 8192], P('vocab', 'width'), may hold values from -0.0003376007 to 0.0003376007
- emb_second: float32 [4800], P('vocab'), may hold values from 3.8146974e-09 to 3.8146972e-08
- head_first: bfloat16 [4800, 8192], P('vocab', 'width'), may hold values from -0.0003376007 to 0.0003376007
- head_second: float32 [4800], P('vocab'), may hold values from 3.8146974e-09 to 3.8146972e-08
- step: int32 [1], replicated, may hold values from 1 to 19
Outputs:
- emb_update: bfloat16 [4800, 8192], P('vocab', 'width')
- head_update: bfloat16 [4800, 8192], P('vocab', 'width')
The draws below stay inside these ranges and needn't reach their ends.
Inputs may be any that keep to these rules, and one draw needn't show every extreme that they name: `token_ids`: among the 52 tokens of one index of vocab, at most 8 name rows in the block of 600 rows held by one index of vocab; in every draw some block receives exactly 8 from every index.
All inputs are finite; a program needn't handle non-finite values.
Results may differ from the reference program's by a relative error of at most 0.001.
Values may be sent and summed in bfloat16 or wider, within the bound.
No kernel may reach another device: no remote copies, remote signals or barrier semaphores. Data moves between devices by JAX's collectives and lax.ppermute only.
A program may use at most 192 MiB of HBM per device.

```python
import math
import jax
import jax.numpy as jnp
from jax import lax

D = 8192
ROWS_DEV = 600
TOK_DEV = 52
VOCAB = 4800
TOKENS = 416
CAP = 8
N_VOCAB = 8


def draw_token_ids(key, part):
    base = jax.random.fold_in(key, 7)
    target_block = jax.random.randint(jax.random.fold_in(base, 1), (), 0, N_VOCAB)
    others = jnp.arange((N_VOCAB - 1) * CAP, dtype=jnp.int32) // CAP
    others = others + (others >= target_block).astype(jnp.int32)

    def one_block(index):
        block_key = jax.random.fold_in(base, index + 2)
        picked = jax.random.permutation(jax.random.fold_in(block_key, 1), others)[:TOK_DEV - CAP]
        owner_list = jnp.concatenate([picked, jnp.full((CAP,), target_block, jnp.int32)])
        owner_list = jax.random.permutation(jax.random.fold_in(block_key, 2), owner_list)
        within = jax.random.randint(jax.random.fold_in(block_key, 3), (TOK_DEV,), 0, ROWS_DEV)
        return owner_list * ROWS_DEV + within
    return jax.vmap(one_block)(jnp.arange(N_VOCAB, dtype=jnp.int32)).reshape(TOKENS)


def draw_logit_cot(key, part):
    base = jax.random.fold_in(key, 13)
    position = jnp.arange(VOCAB, dtype=jnp.float32) / VOCAB
    spread = jnp.exp(jax.random.uniform(jax.random.fold_in(base, 2), (VOCAB,), jnp.float32) * math.log(10.0))
    noise = jnp.clip(jax.random.normal(jax.random.fold_in(base, 1), (TOKENS, VOCAB), jnp.float32), -6.0, 6.0)
    ramp = jnp.exp(position * math.log(2.5))
    return (noise * (spread * ramp)[None, :] / (4.0 * math.sqrt(VOCAB))).astype(jnp.bfloat16)


def steps_of(key, extent, cuts, low, top_value):
    factor_of, own = 1.0, jax.random.fold_in(key, 6)
    for axis_at, shards_of in cuts:
        draws = jnp.exp(jax.random.uniform(jax.random.fold_in(own, axis_at), (shards_of,), jnp.float32, low / len(cuts), top_value / len(cuts)))
        factor_of = factor_of * jnp.repeat(draws, extent[axis_at] // shards_of).reshape([-1 if axis == axis_at else 1 for axis in range(len(extent))])
    return factor_of


def normal_values(rng, extent, deviation, limit, split=(), kind=jnp.bfloat16):
    drawn = jax.random.normal(rng, extent, jnp.float32) * deviation
    if len(split) > 0:
        drawn = steps_of(rng, extent, split, -0.22, 0.18) * drawn
    return jnp.clip(drawn, min=-limit, max=limit).astype(kind)


def setup_inputs(seed: int = 0) -> dict:
    streams_of = jax.random.split(jax.random.key(seed), 10)
    return {
        "token_ids": draw_token_ids(jax.random.fold_in(streams_of[9], 71), 0),
        "hidden": normal_values(streams_of[1], (TOKENS, D), 1.0, 6.0, ((0, 8), (1, 4))),
        "embed_cot": normal_values(streams_of[2], (TOKENS, D), 1.0, 6.0, ((0, 8), (1, 4))),
        "logit_cot": draw_logit_cot(jax.random.fold_in(streams_of[9], 71), 0),
        "emb_first": normal_values(streams_of[4], (VOCAB, D), ((8 * VOCAB * D) ** -0.5), 0.0003376007, ((0, 8), (1, 4))),
        "emb_second": jnp.clip(jnp.exp(math.log(3.814697180359872e-08) - 2.30258502 * jax.random.uniform(streams_of[5], (VOCAB,), jnp.float32) ** steps_of(streams_of[5], (VOCAB,), ((0, 8),), -0.2, 0.2)), 3.814697446813398e-09, 3.814697180359872e-08),
        "head_first": normal_values(streams_of[6], (VOCAB, D), ((8 * VOCAB * D) ** -0.5), 0.0003376007, ((0, 8), (1, 4))),
        "head_second": jnp.clip(jnp.exp(math.log(3.814697180359872e-08) - 2.30258502 * jax.random.uniform(streams_of[7], (VOCAB,), jnp.float32) ** steps_of(streams_of[7], (VOCAB,), ((0, 8),), -0.2, 0.2)), 3.814697446813398e-09, 3.814697180359872e-08),
        "step": jax.random.randint(streams_of[8], (1,), 1, 20).astype(jnp.int32),
    }


def adam_rows(grad, rows, first, second, clip, corr1, corr2):
    moved = 0.9 * first.astype(jnp.float32) + 0.1 * (clip * grad)
    kept = 0.95 * second + 0.05 * (clip * clip) * rows / D
    return (moved / corr1 / (jnp.sqrt(kept / corr2)[:, None] + 1e-08)).astype(jnp.bfloat16)

def reference(token_ids, hidden, embed_cot, logit_cot, emb_first, emb_second, head_first, head_second, step):
    head_grad = jnp.dot(logit_cot.T, hidden, preferred_element_type=jnp.float32)
    emb_grad = jax.ops.segment_sum(embed_cot.astype(jnp.float32), token_ids, num_segments=VOCAB)
    emb_rows = lax.optimization_barrier(jnp.sum(emb_grad * emb_grad, axis=1))
    head_rows = lax.optimization_barrier(jnp.sum(head_grad * head_grad, axis=1))
    total = jnp.sum(emb_rows) + jnp.sum(head_rows)
    clip = 1.0 / (jnp.sqrt(total) + 1e-06)
    count = step[0].astype(jnp.float32)
    corr1 = 1.0 - jnp.power(jnp.float32(0.9), count)
    corr2 = 1.0 - jnp.power(jnp.float32(0.95), count)
    emb_update = adam_rows(emb_grad, emb_rows, emb_first, emb_second, clip, corr1, corr2)
    head_update = adam_rows(head_grad, head_rows, head_first, head_second, clip, corr1, corr2)
    return (emb_update, head_update)
```

```python
import functools

import jax
import jax.numpy as jnp
from jax import lax
from jax.experimental import pallas as pl
from jax.experimental.pallas import tpu as pltpu
from jax.sharding import PartitionSpec as P


LANES = 128


def round_up(value, multiple):
    return (value + multiple - 1) // multiple * multiple


def swap(x, axis, distance):
    return lax.ppermute(x, axis, [(i, i ^ distance) for i in range(lax.axis_size(axis))])


def token_slots(token_ids, index, owner_count, tok_count, row_count, slot_count):
    own = lax.dynamic_slice_in_dim(token_ids, index * tok_count, tok_count, 0)
    owner = own // row_count
    place = jnp.arange(tok_count, dtype=jnp.int32)
    earlier = (owner[:, None] == owner[None, :]) & (place[None, :] < place[:, None])
    order = jnp.sum(earlier.astype(jnp.int32), axis=1)
    send_slot = (owner ^ index) * slot_count + order
    blocks = token_ids.reshape(owner_count, tok_count) - index * row_count
    ours = (blocks >= 0) & (blocks < row_count)
    before = ours[:, None, :] & (place[None, None, :] < place[None, :, None])
    position = jnp.sum(before.astype(jnp.int32), axis=2)
    source = jnp.arange(owner_count, dtype=jnp.int32)[:, None] ^ index
    slot = jnp.where(ours, source * slot_count + position, -1).reshape(-1)
    wanted = jnp.arange(owner_count * slot_count, dtype=jnp.int32)
    hit = slot[None, :] == wanted[:, None]
    slot_row = jnp.sum(jnp.where(hit, blocks.reshape(1, -1) + 1, 0), axis=1) - 1
    return send_slot, slot_row


def row_sums(squares, spare):
    spare[...] = jnp.zeros_like(spare)
    spare[: squares.shape[0], :] = squares
    return jnp.sum(spare[...].T, axis=0, keepdims=True)


def fold(square):
    total = square[:, :LANES]
    for start in range(LANES, square.shape[1], LANES):
        total = total + square[:, start : start + LANES]
    return total


def norms_kernel(groups, tok, depth, step_cols, where_ref, slot_row_ref, *refs):
    hid = refs[: 2 * groups]
    logit = refs[2 * groups : 3 * groups]
    emb = refs[3 * groups : 4 * groups]
    stats_ref, left_ref, right_ref, pick_ref, emb_ref = refs[4 * groups : 4 * groups + 5]
    logit_buf, left_buf, spare = refs[4 * groups + 5 :]
    rows = left_ref.shape[0]
    columns = right_ref.shape[1]
    minor, first_group = where_ref[0], where_ref[1]
    for j in range(groups):
        logit_buf[j] = logit[j][...]
    left_buf[...] = jnp.zeros_like(left_buf)
    right_ref[...] = jnp.zeros_like(right_ref)
    for k in range(groups):
        block = logit_buf[first_group ^ k]
        low, high = block[:tok, :], block[tok:, :]
        is_low = minor == 0
        left_buf[2 * k * depth : 2 * k * depth + tok, :] = jnp.where(is_low, low, high)
        left_buf[(2 * k + 1) * depth : (2 * k + 1) * depth + tok, :] = jnp.where(is_low, high, low)
        for part in range(2):
            start = (2 * k + part) * depth
            right_ref[start : start + tok, :] = hid[2 * k + part][...]
    left_ref[...] = left_buf[...].T
    slots = emb_ref.shape[0]
    each = slots // groups
    for k in range(groups):
        emb_ref[k * each : (k + 1) * each, :] = emb[k][...]
    row_of = lax.broadcasted_iota(jnp.int32, (rows, slots), 0)
    pick_ref[...] = (row_of == slot_row_ref[...]).astype(jnp.float32).astype(jnp.bfloat16)
    head_squares = jnp.zeros((rows, LANES), jnp.float32)
    emb_squares = jnp.zeros((rows, LANES), jnp.float32)
    for start in range(0, columns, step_cols):
        cols = slice(start, start + step_cols)
        grad = jnp.dot(left_ref[...], right_ref[:, cols], preferred_element_type=jnp.float32)
        head_squares = head_squares + fold(grad * grad)
        grad = jnp.dot(pick_ref[...], emb_ref[:, cols], preferred_element_type=jnp.float32)
        emb_squares = emb_squares + fold(grad * grad)
    head_rows = row_sums(head_squares, spare)
    emb_rows = row_sums(emb_squares, spare)
    total = jnp.sum(head_rows + emb_rows, axis=1, keepdims=True)
    stats_ref[...] = jnp.zeros_like(stats_ref)
    stats_ref[0:1, :] = head_rows
    stats_ref[1:2, :] = emb_rows
    stats_ref[2:3, :] = jnp.broadcast_to(total, head_rows.shape)


def update_kernel(width_total, scalar_ref, stats_ref, total_ref, second_ref, left_ref, right_ref, pick_ref, emb_ref,
                  emb_first_ref, head_first_ref, emb_out_ref, head_out_ref, head_scale, emb_scale):
    rows = left_ref.shape[0]
    total = total_ref[0:1, :]
    clip = 1.0 / (jnp.sqrt(total) + 1e-06)

    @pl.when(pl.program_id(0) == 0)
    def _():
        corr1, corr2 = scalar_ref[0], scalar_ref[1]
        clip_row = clip[:, 0:1]
        for at, scale in ((0, head_scale), (1, emb_scale)):
            kept = 0.95 * second_ref[at : at + 1, :] + 0.05 * (clip_row * clip_row) * stats_ref[at : at + 1, :] / width_total
            inverse = 1.0 / (corr1 * (jnp.sqrt(kept / corr2) + 1e-08))
            scale[...] = jnp.broadcast_to(inverse, (LANES, inverse.shape[1])).T

    cols = emb_first_ref.shape[1]
    factor = 0.1 * clip
    for left, right, first, scale, out in (
        (pick_ref, emb_ref, emb_first_ref, emb_scale, emb_out_ref),
        (left_ref, right_ref, head_first_ref, head_scale, head_out_ref),
    ):
        grad = jnp.dot(left[...], right[...], preferred_element_type=jnp.float32)
        for start in range(0, cols, LANES):
            at = slice(start, start + LANES)
            moved = 0.9 * first[:, at].astype(jnp.float32) + factor * grad[:, at]
            out[:, at] = (moved * scale[:rows, :]).astype(jnp.bfloat16)


def whole():
    return pl.BlockSpec(memory_space=pltpu.VMEM)


def paired(token_ids, hidden, embed_cot, logit_cot, emb_first, emb_second, head_first, head_second, step):
    rows, columns = emb_first.shape
    tok = hidden.shape[0]
    owners, groups = lax.axis_size("vocab"), lax.axis_size("width")
    width_total = columns * groups
    index, column_index = lax.axis_index("vocab"), lax.axis_index("width")
    slot_count = (tok + owners - 1) // owners + 1
    send_slot, slot_row = token_slots(token_ids, index, owners, tok, rows, slot_count)
    slots = owners * slot_count
    chosen = (send_slot[None, :] == jnp.arange(slots, dtype=jnp.int32)[:, None]).astype(jnp.bfloat16)
    outbox = jnp.dot(chosen, embed_cot, preferred_element_type=jnp.bfloat16).reshape(groups, 2, slot_count, columns)

    hid = [None] * (2 * groups)
    hid[0] = hidden
    hid[1] = swap(hidden, "vocab", 1)
    across = swap(outbox[:, 1].reshape(groups * slot_count, columns), "vocab", 1).reshape(groups, slot_count, columns)
    for k in range(1, groups):
        hid[2 * k] = swap(hidden, "vocab", 2 * k)
    logit = [logit_cot]
    for j in range(1, groups):
        logit.append(swap(logit[j - 1], "width", 1) if j & 1 else swap(logit_cot, "width", j))
    emb = []
    for k in range(groups):
        pair = jnp.concatenate([outbox[k, 0], across[k]], axis=0)
        emb.append(pair if k == 0 else swap(pair, "vocab", 2 * k))
    for k in range(1, groups):
        hid[2 * k + 1] = swap(hid[2 * k], "vocab", 1)

    depth = round_up(tok, 64)
    lanes = round_up(rows, LANES)
    where = jnp.stack([index & 1, (index >> 1) ^ column_index]).astype(jnp.int32)
    stats, left, right, pick, emb_all = pl.pallas_call(
        functools.partial(norms_kernel, groups, tok, depth, 512),
        out_shape=(
            jax.ShapeDtypeStruct((4, lanes), jnp.float32),
            jax.ShapeDtypeStruct((rows, 2 * groups * depth), jnp.bfloat16),
            jax.ShapeDtypeStruct((2 * groups * depth, columns), jnp.bfloat16),
            jax.ShapeDtypeStruct((rows, slots), jnp.bfloat16),
            jax.ShapeDtypeStruct((slots, columns), jnp.bfloat16),
        ),
        in_specs=[pl.BlockSpec(memory_space=pltpu.SMEM)] + [whole()] * (1 + 4 * groups),
        out_specs=(whole(),) * 5,
        scratch_shapes=[
            pltpu.VMEM((groups,) + logit_cot.shape, jnp.bfloat16),
            pltpu.VMEM((2 * groups * depth, rows), jnp.bfloat16),
            pltpu.VMEM((lanes, LANES), jnp.float32),
        ],
        compiler_params=pltpu.CompilerParams(vmem_limit_bytes=32 * 1024 * 1024),
        name="norms",
    )(where, slot_row[None, :], *hid, *logit, *emb)

    distance = 1
    while distance < groups:
        stats = stats + swap(stats, "width", distance)
        distance *= 2
    total = stats[2:3, :LANES]
    distance = 1
    while distance < owners:
        total = total + swap(total, "vocab", distance)
        distance *= 2

    count = step[0].astype(jnp.float32)
    corr1 = 1.0 - jnp.power(jnp.float32(0.9), count)
    corr2 = 1.0 - jnp.power(jnp.float32(0.95), count)
    second = jnp.pad(jnp.stack([head_second, emb_second]), ((0, 0), (0, lanes - rows)), constant_values=1.0)
    step_cols = 512
    tile = pl.BlockSpec((rows, step_cols), lambda i: (0, i))
    emb_update, head_update = pl.pallas_call(
        functools.partial(update_kernel, float(width_total)),
        grid=(columns // step_cols,),
        out_shape=(jax.ShapeDtypeStruct((rows, columns), jnp.bfloat16),) * 2,
        in_specs=[
            pl.BlockSpec(memory_space=pltpu.SMEM), whole(), whole(), whole(), whole(),
            pl.BlockSpec((right.shape[0], step_cols), lambda i: (0, i)), whole(),
            pl.BlockSpec((slots, step_cols), lambda i: (0, i)),
            tile, tile,
        ],
        out_specs=(tile, tile),
        scratch_shapes=[pltpu.VMEM((lanes, LANES), jnp.float32)] * 2,
        compiler_params=pltpu.CompilerParams(vmem_limit_bytes=32 * 1024 * 1024),
        name="update",
    )(jnp.stack([corr1, corr2]), stats, total, second, left, right, pick, emb_all, emb_first, head_first)
    return emb_update, head_update


def adam_rows(grad, rows, first, second, clip, corr1, corr2, width_total):
    moved = 0.9 * first.astype(jnp.float32) + 0.1 * (clip * grad)
    kept = 0.95 * second + 0.05 * (clip * clip) * rows / width_total
    return (moved / corr1 / (jnp.sqrt(kept / corr2)[:, None] + 1e-08)).astype(jnp.bfloat16)


def general(token_ids, hidden, embed_cot, logit_cot, emb_first, emb_second, head_first, head_second, step):
    row_count, columns = emb_first.shape
    tok_count = hidden.shape[0]
    owner_count = lax.axis_size("vocab")
    width_total = columns * lax.axis_size("width")
    own_index = lax.axis_index("vocab")
    head_grad = lax.dot_general(
        lax.all_gather(logit_cot, "width", axis=0, tiled=True),
        lax.all_gather(hidden, "vocab", axis=0, tiled=True),
        (((0,), (0,)), ((), ())),
        preferred_element_type=jnp.float32,
    )
    slot_count = (tok_count + owner_count - 1) // owner_count + 1
    own_ids = lax.dynamic_slice_in_dim(token_ids, own_index * tok_count, tok_count, 0)
    dest_owner = own_ids // row_count
    chosen = (dest_owner[:, None] == jnp.arange(owner_count, dtype=jnp.int32)[None, :]).astype(jnp.int32)
    order_in = jnp.sum(jnp.cumsum(chosen, axis=0) * chosen, axis=1) - 1
    target_slot = dest_owner * slot_count + order_in
    outbox = jnp.zeros((owner_count * slot_count, columns), jnp.bfloat16).at[target_slot].set(embed_cot)
    arrived = lax.all_to_all(outbox, "vocab", split_axis=0, concat_axis=0, tiled=True)
    all_blocks = token_ids.reshape(owner_count, tok_count) - own_index * row_count
    ours = ((all_blocks >= 0) & (all_blocks < row_count)).astype(jnp.int32)
    slot_index = jnp.arange(owner_count, dtype=jnp.int32)[:, None] * slot_count + jnp.cumsum(ours, axis=1) - 1
    slot_index = jnp.where(ours > 0, slot_index, owner_count * slot_count)
    slot_row = jnp.full((owner_count * slot_count,), row_count, jnp.int32)
    slot_row = slot_row.at[slot_index.reshape(-1)].set(all_blocks.reshape(-1), mode="drop")
    emb_grad = jnp.zeros((row_count, columns), jnp.float32).at[slot_row].add(arrived.astype(jnp.float32), mode="drop")
    emb_rows, head_rows = lax.psum(
        (jnp.sum(emb_grad * emb_grad, axis=1), jnp.sum(head_grad * head_grad, axis=1)), "width"
    )
    total = lax.psum(jnp.sum(emb_rows) + jnp.sum(head_rows), "vocab")
    clip = 1.0 / (jnp.sqrt(total) + 1e-06)
    count = step[0].astype(jnp.float32)
    corr1 = 1.0 - jnp.power(jnp.float32(0.9), count)
    corr2 = 1.0 - jnp.power(jnp.float32(0.95), count)
    return (
        adam_rows(emb_grad, emb_rows, emb_first, emb_second, clip, corr1, corr2, width_total),
        adam_rows(head_grad, head_rows, head_first, head_second, clip, corr1, corr2, width_total),
    )


def solution(mesh):
    owners, groups = mesh.shape["vocab"], mesh.shape["width"]
    paired_up = owners == 2 * groups and groups & (groups - 1) == 0
    placed = (
        P(),
        P("vocab", "width"),
        P("vocab", "width"),
        P("width", "vocab"),
        P("vocab", "width"),
        P("vocab"),
        P("vocab", "width"),
        P("vocab"),
        P(),
    )
    return jax.shard_map(
        paired if paired_up else general,
        mesh=mesh,
        in_specs=placed,
        out_specs=(P("vocab", "width"), P("vocab", "width")),
        check_vma=False,
    )
```

```python
import functools

import jax
import jax.numpy as jnp
from jax import lax
from jax.experimental import pallas as pl
from jax.experimental.pallas import tpu as pltpu
from jax.sharding import PartitionSpec as P


LANES = 128


def round_up(value, multiple):
    return (value + multiple - 1) // multiple * multiple


def swap(x, axis, distance):
    return lax.ppermute(x, axis, [(i, i ^ distance) for i in range(lax.axis_size(axis))])


def row_sums(squares, spare):
    spare[...] = jnp.zeros_like(spare)
    spare[: squares.shape[0], :] = squares
    return jnp.sum(spare[...].T, axis=0, keepdims=True)


def fold(square):
    total = square[:, :LANES]
    for start in range(LANES, square.shape[1], LANES):
        total = total + square[:, start : start + LANES]
    return total


def pack_kernel(rows, groups, slot_count, ids_ref, cot_hbm, near_ref, far_ref, slot_row_ref, cot_ref, sem):
    fetch = pltpu.make_async_copy(cot_hbm, cot_ref, sem)
    fetch.start()
    owners, tok = ids_ref.shape
    slots = owners * slot_count
    index = lax.axis_index("vocab")
    owner = lax.broadcasted_iota(jnp.int32, (owners, tok), 0)
    relative = owner ^ index
    before = lax.broadcasted_iota(jnp.int32, (tok, tok), 0) < lax.broadcasted_iota(jnp.int32, (tok, tok), 1)
    before = before.astype(jnp.float32).astype(jnp.bfloat16)

    def order_of(member):
        return jnp.dot(member.astype(jnp.float32).astype(jnp.bfloat16), before, preferred_element_type=jnp.float32)

    own = ids_ref[pl.ds(index, 1), :]
    to_owner = (own >= owner * rows) & (own < owner * rows + rows)
    first_slot = ((relative & 1) * groups + (relative >> 1)) * slot_count
    slot = jnp.sum(jnp.where(to_owner, first_slot.astype(jnp.float32) + order_of(to_owner), 0.0), axis=0, keepdims=True)
    wanted = lax.broadcasted_iota(jnp.int32, (slots, tok), 0).astype(jnp.float32)
    chosen = (wanted == slot).astype(jnp.float32).astype(jnp.bfloat16)
    half = slots // 2
    fetch.wait()
    near_ref[...] = jnp.dot(chosen[:half], cot_ref[...], preferred_element_type=jnp.float32).astype(jnp.bfloat16)
    far_ref[...] = jnp.dot(chosen[half:], cot_ref[...], preferred_element_type=jnp.float32).astype(jnp.bfloat16)

    local = ids_ref[...] - index * rows
    ours = (local >= 0) & (local < rows)
    slot = jnp.where(ours, (relative * slot_count).astype(jnp.float32) + order_of(ours), -1.0)
    local = local.astype(jnp.float32) + 1.0
    row = jnp.zeros((slots, 1), jnp.float32)
    for source in range(owners):
        hit = wanted == slot[source : source + 1, :]
        row = row + jnp.sum(jnp.where(hit, local[source : source + 1, :], 0.0), axis=1, keepdims=True)
    slot_row_ref[...] = jnp.broadcast_to(row - 1.0, (slots, LANES)).T[0:1, :]


def merge_kernel(groups, slot_count, near_ref, far_ref, *pair_refs):
    for k in range(groups):
        at = slice(k * slot_count, (k + 1) * slot_count)
        pair_refs[k][:slot_count, :] = near_ref[at, :]
        pair_refs[k][slot_count:, :] = far_ref[at, :]


def partial_kernel(groups, tok, depth, step_cols, *refs):
    early = 2 * (groups - 1)
    hid, logit = refs[:early], refs[early : early + groups]
    emb_first_ref, head_first_ref = refs[early + groups : early + groups + 2]
    grad_ref, last_ref, emb_copy_ref, head_copy_ref = refs[early + groups + 2 : early + groups + 6]
    logit_buf, own_ref, left_buf, left_ref, right_ref, sems = refs[early + groups + 6 :]
    own_tokens = pltpu.make_async_copy(hid[0], own_ref, sems.at[2])
    own_logits = pltpu.make_async_copy(logit[0], logit_buf.at[0], sems.at[3])
    copies = [
        pltpu.make_async_copy(emb_first_ref, emb_copy_ref, sems.at[0]),
        pltpu.make_async_copy(head_first_ref, head_copy_ref, sems.at[1]),
    ]
    for copy in [own_tokens, own_logits] + copies:
        copy.start()
    index, column_index = lax.axis_index("vocab"), lax.axis_index("width")
    is_low = (index & 1) == 0
    first_group = (index >> 1) ^ column_index
    for j in range(1, groups):
        logit_buf[j] = logit[j][...]
    left_buf[...] = jnp.zeros_like(left_buf)
    right_ref[...] = jnp.zeros_like(right_ref)
    for at in range(1, early):
        right_ref[at * depth : at * depth + tok, :] = hid[at][...]
    own_tokens.wait()
    right_ref[:tok, :] = own_ref[...]
    own_logits.wait()
    for k in range(groups):
        block = logit_buf[first_group ^ k]
        low, high = block[:tok, :], block[tok:, :]
        left_buf[2 * k * depth : 2 * k * depth + tok, :] = jnp.where(is_low, low, high)
        left_buf[(2 * k + 1) * depth : (2 * k + 1) * depth + tok, :] = jnp.where(is_low, high, low)
    left_ref[...] = left_buf[: early * depth, :].T
    last_ref[...] = left_buf[early * depth :, :].T
    for start in range(0, grad_ref.shape[1], step_cols):
        cols = slice(start, start + step_cols)
        grad_ref[:, cols] = jnp.dot(left_ref[...], right_ref[:, cols], preferred_element_type=jnp.float32)
    for copy in copies:
        copy.wait()


def embed_kernel(groups, step_cols, slot_row_ref, *refs):
    pairs = refs[:groups]
    rows_ref, pick_ref, emb_ref, spare = refs[groups:]
    rows, slots = pick_ref.shape
    each = slots // groups
    for k in range(groups):
        emb_ref[k * each : (k + 1) * each, :] = pairs[k][...]
    row_of = lax.broadcasted_iota(jnp.int32, (rows, slots), 0).astype(jnp.float32)
    pick_ref[...] = (row_of == slot_row_ref[...]).astype(jnp.float32).astype(jnp.bfloat16)
    squares = jnp.zeros((rows, LANES), jnp.float32)
    for start in range(0, emb_ref.shape[1], step_cols):
        grad = jnp.dot(pick_ref[...], emb_ref[:, start : start + step_cols], preferred_element_type=jnp.float32)
        squares = squares + fold(grad * grad)
    rows_ref[...] = row_sums(squares, spare)


def norms_kernel(tok, depth, step_cols, near_ref, far_ref, last_ref, part_ref, emb_rows_ref, stats_ref, grad_ref, right_ref, spare):
    right_ref[...] = jnp.zeros_like(right_ref)
    right_ref[:tok, :] = near_ref[...]
    right_ref[depth : depth + tok, :] = far_ref[...]
    rows, columns = grad_ref.shape
    squares = jnp.zeros((rows, LANES), jnp.float32)
    for start in range(0, columns, step_cols):
        cols = slice(start, start + step_cols)
        grad = part_ref[:, cols] + jnp.dot(last_ref[...], right_ref[:, cols], preferred_element_type=jnp.float32)
        grad_ref[:, cols] = grad
        squares = squares + fold(grad * grad)
    head_rows = row_sums(squares, spare)
    emb_rows = emb_rows_ref[...]
    total = jnp.sum(head_rows + emb_rows, axis=1, keepdims=True)
    stats_ref[...] = jnp.zeros_like(stats_ref)
    stats_ref[0:1, :] = head_rows
    stats_ref[1:2, :] = emb_rows
    stats_ref[2:3, :] = jnp.broadcast_to(total, head_rows.shape)


def update_kernel(width_total, scalar_ref, stats_ref, total_ref, second_ref, grad_ref, pick_ref, emb_ref,
                  emb_first_ref, head_first_ref, emb_out_ref, head_out_ref, head_scale, emb_scale):
    clip = 1.0 / (jnp.sqrt(total_ref[0:1, :]) + 1e-06)

    @pl.when(pl.program_id(0) == 0)
    def _():
        corr1, corr2 = scalar_ref[0], scalar_ref[1]
        clip_row = clip[:, 0:1]
        for at, scale in ((0, head_scale), (1, emb_scale)):
            kept = 0.95 * second_ref[at : at + 1, :] + 0.05 * (clip_row * clip_row) * stats_ref[at : at + 1, :] / width_total
            inverse = 1.0 / (corr1 * (jnp.sqrt(kept / corr2) + 1e-08))
            scale[...] = jnp.broadcast_to(inverse, (LANES, inverse.shape[1])).T

    tile_rows, columns = emb_out_ref.shape
    at_rows = pl.ds(pl.multiple_of(pl.program_id(0) * tile_rows, 8), tile_rows)
    factor = 0.1 * clip
    emb_by_row, head_by_row = emb_scale[at_rows, :], head_scale[at_rows, :]
    emb_grad = jnp.dot(pick_ref[at_rows, :], emb_ref[...], preferred_element_type=jnp.float32)
    for start in range(0, columns, LANES):
        at = slice(start, start + LANES)
        moved = 0.9 * emb_first_ref[at_rows, at].astype(jnp.float32) + factor * emb_grad[:, at]
        emb_out_ref[:, at] = (moved * emb_by_row).astype(jnp.bfloat16)
        moved = 0.9 * head_first_ref[at_rows, at].astype(jnp.float32) + factor * grad_ref[at_rows, at]
        head_out_ref[:, at] = (moved * head_by_row).astype(jnp.bfloat16)


def whole():
    return pl.BlockSpec(memory_space=pltpu.VMEM)


def keep(array):
    return pltpu.with_memory_space_constraint(array, pltpu.HBM)


def in_hbm():
    return pl.BlockSpec(memory_space=pltpu.HBM)


def tile_of(rows):
    return max([d for d in range(8, 129, 8) if rows % d == 0], default=rows)


def call(kernel, out_shapes, in_specs, scratch, mib, flops, args):
    return pl.pallas_call(
        kernel,
        out_shape=tuple(jax.ShapeDtypeStruct(shape, dtype) for shape, dtype in out_shapes),
        in_specs=in_specs,
        out_specs=tuple(whole() for _ in out_shapes),
        scratch_shapes=scratch,
        compiler_params=pltpu.CompilerParams(vmem_limit_bytes=mib * 1024 * 1024),
        cost_estimate=pl.CostEstimate(flops=flops, bytes_accessed=1024, transcendentals=0),
    )(*args)


def paired(*arrays):
    return paired_body(*arrays)


def paired_body(token_ids, hidden, embed_cot, logit_cot, emb_first, emb_second, head_first, head_second, step):
    rows, columns = emb_first.shape
    tok = hidden.shape[0]
    owners, groups = lax.axis_size("vocab"), lax.axis_size("width")
    width_total = columns * groups
    slot_count = (tok + owners - 1) // owners + 1
    slots = owners * slot_count
    depth = round_up(tok, 64)
    lanes = round_up(rows, LANES)
    bf16, f32 = jnp.bfloat16, jnp.float32

    hid = [hidden] + [None] * (2 * groups - 1)
    logit = [logit_cot] + [None] * (groups - 1)
    logit[1] = swap(logit_cot, "width", 1)
    hid[1] = swap(hidden, "vocab", 1)
    for k in range(1, groups):
        hid[2 * k] = swap(hidden, "vocab", 2 * k)
    near, far, slot_row = call(
        functools.partial(pack_kernel, rows, groups, slot_count),
        (((slots // 2, columns), bf16), ((slots // 2, columns), bf16), ((1, slots), f32)),
        [whole(), in_hbm()], [pltpu.VMEM((tok, columns), bf16), pltpu.SemaphoreType.DMA], 8, 1000000,
        (token_ids.reshape(owners, tok), keep(embed_cot)),
    )
    across = swap(far, "vocab", 1)
    for j in range(2, groups):
        logit[j] = swap(logit[j - 1], "width", 1) if j & 1 else swap(logit_cot, "width", j)
    emb = list(call(
        functools.partial(merge_kernel, groups, slot_count),
        (((2 * slot_count, columns), bf16),) * groups, [whole()] * 2, [], 8, 1000000, (near, across),
    ))
    for k in range(1, groups):
        hid[2 * k + 1] = swap(hid[2 * k], "vocab", 1)
        emb[k] = swap(emb[k], "vocab", 2 * k)

    early = 2 * (groups - 1)
    part, last, emb_near, head_near = call(
        functools.partial(partial_kernel, groups, tok, depth, 512),
        (((rows, columns), f32), ((rows, 2 * depth), bf16), ((rows, columns), bf16), ((rows, columns), bf16)),
        [in_hbm()] + [whole()] * (early - 1) + [in_hbm()] + [whole()] * (groups - 1) + [in_hbm()] * 2,
        [
            pltpu.VMEM((groups,) + logit_cot.shape, bf16),
            pltpu.VMEM((tok, columns), bf16),
            pltpu.VMEM((2 * groups * depth, rows), bf16),
            pltpu.VMEM((rows, early * depth), bf16),
            pltpu.VMEM((early * depth, columns), bf16),
            pltpu.SemaphoreType.DMA((4,)),
        ],
        24, 1000000000, (keep(hidden), *hid[1:early], keep(logit_cot), *logit[1:], keep(emb_first), keep(head_first)),
    )
    emb_rows, pick, emb_all = call(
        functools.partial(embed_kernel, groups, 512),
        (((1, lanes), f32), ((rows, slots), bf16), ((slots, columns), bf16)),
        [whole()] * (1 + groups), [pltpu.VMEM((lanes, LANES), f32)], 16, 100000000, (slot_row, *emb),
    )
    stats, grad = call(
        functools.partial(norms_kernel, tok, depth, 512),
        (((4, lanes), f32), ((rows, columns), f32)),
        [whole()] * 5, [pltpu.VMEM((2 * depth, columns), bf16), pltpu.VMEM((lanes, LANES), f32)], 24, 300000000,
        (hid[early], hid[early + 1], last, part, emb_rows),
    )

    distance = 1
    while distance < groups:
        stats = stats + swap(stats, "width", distance)
        distance *= 2
    total = stats[2:3, :LANES]
    distance = 1
    while distance < owners:
        total = total + swap(total, "vocab", distance)
        distance *= 2

    count = step[0].astype(f32)
    corr1 = 1.0 - jnp.power(f32(0.9), count)
    corr2 = 1.0 - jnp.power(f32(0.95), count)
    second = jnp.pad(jnp.stack([head_second, emb_second]), ((0, 0), (0, lanes - rows)), constant_values=1.0)
    step_rows = tile_of(rows)
    tile = pl.BlockSpec((step_rows, columns), lambda i: (i, 0))
    return pl.pallas_call(
        functools.partial(update_kernel, float(width_total)),
        grid=(rows // step_rows,),
        out_shape=(jax.ShapeDtypeStruct((rows, columns), bf16),) * 2,
        in_specs=[pl.BlockSpec(memory_space=pltpu.SMEM)] + [whole()] * 8,
        out_specs=(tile, tile),
        scratch_shapes=[pltpu.VMEM((lanes, LANES), f32)] * 2,
        compiler_params=pltpu.CompilerParams(vmem_limit_bytes=24 * 1024 * 1024),
        name="update",
    )(jnp.stack([corr1, corr2]), stats, total, second, grad, pick, emb_all, emb_near, head_near)


def adam_rows(grad, rows, first, second, clip, corr1, corr2, width_total):
    moved = 0.9 * first.astype(jnp.float32) + 0.1 * (clip * grad)
    kept = 0.95 * second + 0.05 * (clip * clip) * rows / width_total
    return (moved / corr1 / (jnp.sqrt(kept / corr2)[:, None] + 1e-08)).astype(jnp.bfloat16)


def general(token_ids, hidden, embed_cot, logit_cot, emb_first, emb_second, head_first, head_second, step):
    row_count, columns = emb_first.shape
    tok_count = hidden.shape[0]
    owner_count = lax.axis_size("vocab")
    width_total = columns * lax.axis_size("width")
    own_index = lax.axis_index("vocab")
    head_grad = lax.dot_general(
        lax.all_gather(logit_cot, "width", axis=0, tiled=True),
        lax.all_gather(hidden, "vocab", axis=0, tiled=True),
        (((0,), (0,)), ((), ())),
        preferred_element_type=jnp.float32,
    )
    slot_count = (tok_count + owner_count - 1) // owner_count + 1
    own_ids = lax.dynamic_slice_in_dim(token_ids, own_index * tok_count, tok_count, 0)
    dest_owner = own_ids // row_count
    chosen = (dest_owner[:, None] == jnp.arange(owner_count, dtype=jnp.int32)[None, :]).astype(jnp.int32)
    order_in = jnp.sum(jnp.cumsum(chosen, axis=0) * chosen, axis=1) - 1
    target_slot = dest_owner * slot_count + order_in
    outbox = jnp.zeros((owner_count * slot_count, columns), jnp.bfloat16).at[target_slot].set(embed_cot)
    arrived = lax.all_to_all(outbox, "vocab", split_axis=0, concat_axis=0, tiled=True)
    all_blocks = token_ids.reshape(owner_count, tok_count) - own_index * row_count
    ours = ((all_blocks >= 0) & (all_blocks < row_count)).astype(jnp.int32)
    slot_index = jnp.arange(owner_count, dtype=jnp.int32)[:, None] * slot_count + jnp.cumsum(ours, axis=1) - 1
    slot_index = jnp.where(ours > 0, slot_index, owner_count * slot_count)
    slot_row = jnp.full((owner_count * slot_count,), row_count, jnp.int32)
    slot_row = slot_row.at[slot_index.reshape(-1)].set(all_blocks.reshape(-1), mode="drop")
    emb_grad = jnp.zeros((row_count, columns), jnp.float32).at[slot_row].add(arrived.astype(jnp.float32), mode="drop")
    emb_rows, head_rows = lax.psum(
        (jnp.sum(emb_grad * emb_grad, axis=1), jnp.sum(head_grad * head_grad, axis=1)), "width"
    )
    total = lax.psum(jnp.sum(emb_rows) + jnp.sum(head_rows), "vocab")
    clip = 1.0 / (jnp.sqrt(total) + 1e-06)
    count = step[0].astype(jnp.float32)
    corr1 = 1.0 - jnp.power(jnp.float32(0.9), count)
    corr2 = 1.0 - jnp.power(jnp.float32(0.95), count)
    return (
        adam_rows(emb_grad, emb_rows, emb_first, emb_second, clip, corr1, corr2, width_total),
        adam_rows(head_grad, head_rows, head_first, head_second, clip, corr1, corr2, width_total),
    )


def solution(mesh):
    owners, groups = mesh.shape["vocab"], mesh.shape["width"]
    paired_up = groups == 4 and owners == 2 * groups
    placed = (
        P(),
        P("vocab", "width"),
        P("vocab", "width"),
        P("width", "vocab"),
        P("vocab", "width"),
        P("vocab"),
        P("vocab", "width"),
        P("vocab"),
        P(),
    )
    return jax.shard_map(
        paired if paired_up else general,
        mesh=mesh,
        in_specs=placed,
        out_specs=(P("vocab", "width"), P("vocab", "width")),
        check_vma=False,
    )
```

```python
import functools

import jax
import jax.numpy as jnp
from jax import lax
from jax.experimental import pallas as pl
from jax.experimental.pallas import tpu as pltpu
from jax.sharding import PartitionSpec as P


LANES = 128


def round_up(value, multiple):
    return (value + multiple - 1) // multiple * multiple


def swap(x, axis, distance):
    return lax.ppermute(x, axis, [(i, i ^ distance) for i in range(lax.axis_size(axis))])


def row_sums(squares, spare):
    spare[...] = jnp.zeros_like(spare)
    spare[: squares.shape[0], :] = squares
    return jnp.sum(spare[...].T, axis=0, keepdims=True)


def fold(square):
    total = square[:, :LANES]
    for start in range(LANES, square.shape[1], LANES):
        total = total + square[:, start : start + LANES]
    return total


def pack_kernel(rows, groups, slot_count, ids_ref, cot_hbm, near_ref, far_ref, slot_row_ref, cot_ref, sem):
    fetch = pltpu.make_async_copy(cot_hbm, cot_ref, sem)
    fetch.start()
    owners, tok = ids_ref.shape
    slots = owners * slot_count
    index = lax.axis_index("vocab")
    owner = lax.broadcasted_iota(jnp.int32, (owners, tok), 0)
    relative = owner ^ index
    before = lax.broadcasted_iota(jnp.int32, (tok, tok), 0) < lax.broadcasted_iota(jnp.int32, (tok, tok), 1)
    before = before.astype(jnp.float32).astype(jnp.bfloat16)

    def order_of(member):
        return jnp.dot(member.astype(jnp.float32).astype(jnp.bfloat16), before, preferred_element_type=jnp.float32)

    own = ids_ref[pl.ds(index, 1), :]
    to_owner = (own >= owner * rows) & (own < owner * rows + rows)
    first_slot = ((relative & 1) * groups + (relative >> 1)) * slot_count
    slot = jnp.sum(jnp.where(to_owner, first_slot.astype(jnp.float32) + order_of(to_owner), 0.0), axis=0, keepdims=True)
    wanted = lax.broadcasted_iota(jnp.int32, (slots, tok), 0).astype(jnp.float32)
    chosen = (wanted == slot).astype(jnp.float32).astype(jnp.bfloat16)
    half = slots // 2
    fetch.wait()
    near_ref[...] = jnp.dot(chosen[:half], cot_ref[...], preferred_element_type=jnp.float32).astype(jnp.bfloat16)
    far_ref[...] = jnp.dot(chosen[half:], cot_ref[...], preferred_element_type=jnp.float32).astype(jnp.bfloat16)

    local = ids_ref[...] - index * rows
    ours = (local >= 0) & (local < rows)
    slot = jnp.where(ours, (relative * slot_count).astype(jnp.float32) + order_of(ours), -1.0)
    local = local.astype(jnp.float32) + 1.0
    row = jnp.zeros((slots, 1), jnp.float32)
    for source in range(owners):
        hit = wanted == slot[source : source + 1, :]
        row = row + jnp.sum(jnp.where(hit, local[source : source + 1, :], 0.0), axis=1, keepdims=True)
    slot_row_ref[...] = jnp.broadcast_to(row - 1.0, (slots, LANES)).T[0:1, :]


def merge_kernel(groups, slot_count, near_ref, far_ref, *pair_refs):
    for k in range(groups):
        at = slice(k * slot_count, (k + 1) * slot_count)
        pair_refs[k][:slot_count, :] = near_ref[at, :]
        pair_refs[k][slot_count:, :] = far_ref[at, :]


def partial_kernel(groups, tok, depth, step_cols, *refs):
    early = 2 * (groups - 1)
    hid, logit = refs[:early], refs[early : early + groups]
    emb_first_ref, head_first_ref = refs[early + groups : early + groups + 2]
    grad_ref, last_ref, emb_copy_ref, head_copy_ref = refs[early + groups + 2 : early + groups + 6]
    logit_buf, own_ref, left_buf, left_ref, right_ref, sems = refs[early + groups + 6 :]
    own_tokens = pltpu.make_async_copy(hid[0], own_ref, sems.at[2])
    own_logits = pltpu.make_async_copy(logit[0], logit_buf.at[0], sems.at[3])
    copies = [
        pltpu.make_async_copy(emb_first_ref, emb_copy_ref, sems.at[0]),
        pltpu.make_async_copy(head_first_ref, head_copy_ref, sems.at[1]),
    ]
    for copy in [own_tokens, own_logits] + copies:
        copy.start()
    index, column_index = lax.axis_index("vocab"), lax.axis_index("width")
    is_low = (index & 1) == 0
    first_group = (index >> 1) ^ column_index
    for j in range(1, groups):
        logit_buf[j] = logit[j][...]
    left_buf[...] = jnp.zeros_like(left_buf)
    right_ref[...] = jnp.zeros_like(right_ref)
    for at in range(1, early):
        right_ref[at * depth : at * depth + tok, :] = hid[at][...]
    own_tokens.wait()
    right_ref[:tok, :] = own_ref[...]
    own_logits.wait()
    for k in range(groups):
        block = logit_buf[first_group ^ k]
        low, high = block[:tok, :], block[tok:, :]
        left_buf[2 * k * depth : 2 * k * depth + tok, :] = jnp.where(is_low, low, high)
        left_buf[(2 * k + 1) * depth : (2 * k + 1) * depth + tok, :] = jnp.where(is_low, high, low)
    left_ref[...] = left_buf[: early * depth, :].T
    last_ref[...] = left_buf[early * depth :, :].T
    for start in range(0, grad_ref.shape[1], step_cols):
        cols = slice(start, start + step_cols)
        grad_ref[:, cols] = jnp.dot(left_ref[...], right_ref[:, cols], preferred_element_type=jnp.float32)
    for copy in copies:
        copy.wait()


def embed_kernel(groups, step_cols, slot_row_ref, *refs):
    pairs = refs[:groups]
    rows_ref, pick_ref, emb_ref, spare = refs[groups:]
    rows, slots = pick_ref.shape
    each = slots // groups
    for k in range(groups):
        emb_ref[k * each : (k + 1) * each, :] = pairs[k][...]
    row_of = lax.broadcasted_iota(jnp.int32, (rows, slots), 0).astype(jnp.float32)
    pick_ref[...] = (row_of == slot_row_ref[...]).astype(jnp.float32).astype(jnp.bfloat16)
    squares = jnp.zeros((rows, LANES), jnp.float32)
    for start in range(0, emb_ref.shape[1], step_cols):
        grad = jnp.dot(pick_ref[...], emb_ref[:, start : start + step_cols], preferred_element_type=jnp.float32)
        squares = squares + fold(grad * grad)
    rows_ref[...] = row_sums(squares, spare)


def norms_kernel(tok, depth, step_cols, near_ref, far_ref, last_ref, part_ref, emb_rows_ref, stats_ref, grad_ref, right_ref, spare):
    right_ref[...] = jnp.zeros_like(right_ref)
    right_ref[:tok, :] = near_ref[...]
    right_ref[depth : depth + tok, :] = far_ref[...]
    rows, columns = grad_ref.shape
    squares = jnp.zeros((rows, LANES), jnp.float32)
    for start in range(0, columns, step_cols):
        cols = slice(start, start + step_cols)
        grad = part_ref[:, cols] + jnp.dot(last_ref[...], right_ref[:, cols], preferred_element_type=jnp.float32)
        grad_ref[:, cols] = grad
        squares = squares + fold(grad * grad)
    head_rows = row_sums(squares, spare)
    emb_rows = emb_rows_ref[...]
    total = jnp.sum(head_rows + emb_rows, axis=1, keepdims=True)
    stats_ref[...] = jnp.zeros_like(stats_ref)
    stats_ref[0:1, :] = head_rows
    stats_ref[1:2, :] = emb_rows
    stats_ref[2:3, :] = jnp.broadcast_to(total, head_rows.shape)


def update_kernel(width_total, scalar_ref, stats_ref, total_ref, second_ref, grad_ref, pick_ref, emb_ref,
                  emb_first_ref, head_first_ref, emb_hbm, head_hbm, emb_out, head_out, keep_scale, grad_scale, sems):
    clip = 1.0 / (jnp.sqrt(total_ref[0:1, 0:1]) + 1e-06)
    corr1, corr2 = scalar_ref[0], scalar_ref[1]
    for at in range(2):
        kept = 0.95 * second_ref[at : at + 1, :] + 0.05 * (clip * clip) * stats_ref[at : at + 1, :] / width_total
        inverse = 1.0 / (corr1 * (jnp.sqrt(kept / corr2) + 1e-08))
        by_row = jnp.broadcast_to(inverse, (LANES, inverse.shape[1])).T
        keep_scale[at] = 0.9 * by_row
        grad_scale[at] = (0.1 * clip) * by_row

    rows, columns = emb_out.shape
    chunk = tile_of(rows)
    copies = []
    for step in range(rows // chunk):
        here = slice(step * chunk, (step + 1) * chunk)
        emb_grad = jnp.dot(pick_ref[here, :], emb_ref[...], preferred_element_type=jnp.float32)
        for table, (grad, first, out, target) in enumerate((
            (grad_ref, head_first_ref, head_out, head_hbm),
            (None, emb_first_ref, emb_out, emb_hbm),
        )):
            keep, scale = keep_scale[table, here, :], grad_scale[table, here, :]
            for start in range(0, columns, LANES):
                cols = slice(start, start + LANES)
                part = emb_grad[:, cols] if grad is None else grad[here, cols]
                out[here, cols] = (keep * first[here, cols].astype(jnp.float32) + scale * part).astype(jnp.bfloat16)
            copy = pltpu.make_async_copy(out.at[here, :], target.at[here, :], sems.at[2 * step + table])
            copy.start()
            copies.append(copy)
    for copy in copies:
        copy.wait()


def whole():
    return pl.BlockSpec(memory_space=pltpu.VMEM)


def keep(array):
    return pltpu.with_memory_space_constraint(array, pltpu.HBM)


def in_hbm():
    return pl.BlockSpec(memory_space=pltpu.HBM)


def tile_of(rows):
    return max([d for d in range(8, 129, 8) if rows % d == 0], default=rows)


def call(kernel, out_shapes, in_specs, scratch, mib, flops, args):
    return pl.pallas_call(
        kernel,
        out_shape=tuple(jax.ShapeDtypeStruct(shape, dtype) for shape, dtype in out_shapes),
        in_specs=in_specs,
        out_specs=tuple(whole() for _ in out_shapes),
        scratch_shapes=scratch,
        compiler_params=pltpu.CompilerParams(vmem_limit_bytes=mib * 1024 * 1024),
        cost_estimate=pl.CostEstimate(flops=flops, bytes_accessed=1024, transcendentals=0),
    )(*args)


def paired(*arrays):
    return paired_body(*arrays)


def paired_body(token_ids, hidden, embed_cot, logit_cot, emb_first, emb_second, head_first, head_second, step):
    rows, columns = emb_first.shape
    tok = hidden.shape[0]
    owners, groups = lax.axis_size("vocab"), lax.axis_size("width")
    width_total = columns * groups
    slot_count = (tok + owners - 1) // owners + 1
    slots = owners * slot_count
    depth = round_up(tok, 64)
    lanes = round_up(rows, LANES)
    bf16, f32 = jnp.bfloat16, jnp.float32

    hid = [hidden] + [None] * (2 * groups - 1)
    logit = [logit_cot] + [None] * (groups - 1)
    logit[1] = swap(logit_cot, "width", 1)
    hid[1] = swap(hidden, "vocab", 1)
    for k in range(1, groups):
        low = k & -k
        hid[2 * k] = swap(hid[2 * (k - low)], "vocab", 2 * low)
    near, far, slot_row = call(
        functools.partial(pack_kernel, rows, groups, slot_count),
        (((slots // 2, columns), bf16), ((slots // 2, columns), bf16), ((1, slots), f32)),
        [whole(), in_hbm()], [pltpu.VMEM((tok, columns), bf16), pltpu.SemaphoreType.DMA], 8, 1000000,
        (token_ids.reshape(owners, tok), keep(embed_cot)),
    )
    across = swap(far, "vocab", 1)
    for j in range(2, groups):
        logit[j] = swap(logit[j - 1], "width", 1) if j & 1 else swap(logit_cot, "width", j)
    emb = list(call(
        functools.partial(merge_kernel, groups, slot_count),
        (((2 * slot_count, columns), bf16),) * groups, [whole()] * 2, [], 8, 1000000, (near, across),
    ))
    for k in range(1, groups):
        hid[2 * k + 1] = swap(hid[2 * k], "vocab", 1)
        emb[k] = swap(emb[k], "vocab", 2 * k)

    early = 2 * (groups - 1)
    part, last, emb_near, head_near = call(
        functools.partial(partial_kernel, groups, tok, depth, 512),
        (((rows, columns), f32), ((rows, 2 * depth), bf16), ((rows, columns), bf16), ((rows, columns), bf16)),
        [in_hbm()] + [whole()] * (early - 1) + [in_hbm()] + [whole()] * (groups - 1) + [in_hbm()] * 2,
        [
            pltpu.VMEM((groups,) + logit_cot.shape, bf16),
            pltpu.VMEM((tok, columns), bf16),
            pltpu.VMEM((2 * groups * depth, rows), bf16),
            pltpu.VMEM((rows, early * depth), bf16),
            pltpu.VMEM((early * depth, columns), bf16),
            pltpu.SemaphoreType.DMA((4,)),
        ],
        24, 1000000000, (keep(hidden), *hid[1:early], keep(logit_cot), *logit[1:], keep(emb_first), keep(head_first)),
    )
    emb_rows, pick, emb_all = call(
        functools.partial(embed_kernel, groups, 512),
        (((1, lanes), f32), ((rows, slots), bf16), ((slots, columns), bf16)),
        [whole()] * (1 + groups), [pltpu.VMEM((lanes, LANES), f32)], 16, 100000000, (slot_row, *emb),
    )
    stats, grad = call(
        functools.partial(norms_kernel, tok, depth, 512),
        (((4, lanes), f32), ((rows, columns), f32)),
        [whole()] * 5, [pltpu.VMEM((2 * depth, columns), bf16), pltpu.VMEM((lanes, LANES), f32)], 24, 300000000,
        (hid[early], hid[early + 1], last, part, emb_rows),
    )

    distance = 1
    while distance < groups:
        stats = stats + swap(stats, "width", distance)
        distance *= 2
    total = stats[2:3, :LANES]
    distance = 1
    while distance < owners:
        total = total + swap(total, "vocab", distance)
        distance *= 2

    count = step[0].astype(f32)
    corr1 = 1.0 - jnp.power(f32(0.9), count)
    corr2 = 1.0 - jnp.power(f32(0.95), count)
    second = jnp.pad(jnp.stack([head_second, emb_second]), ((0, 0), (0, lanes - rows)), constant_values=1.0)
    return pl.pallas_call(
        functools.partial(update_kernel, float(width_total)),
        out_shape=(jax.ShapeDtypeStruct((rows, columns), bf16),) * 2,
        in_specs=[pl.BlockSpec(memory_space=pltpu.SMEM)] + [whole()] * 8,
        out_specs=(in_hbm(), in_hbm()),
        scratch_shapes=[
            pltpu.VMEM((rows, columns), bf16),
            pltpu.VMEM((rows, columns), bf16),
            pltpu.VMEM((2, lanes, LANES), f32),
            pltpu.VMEM((2, lanes, LANES), f32),
            pltpu.SemaphoreType.DMA((2 * (rows // tile_of(rows)),)),
        ],
        compiler_params=pltpu.CompilerParams(vmem_limit_bytes=24 * 1024 * 1024),
        name="update",
    )(jnp.stack([corr1, corr2]), stats, total, second, grad, pick, emb_all, emb_near, head_near)


def adam_rows(grad, rows, first, second, clip, corr1, corr2, width_total):
    moved = 0.9 * first.astype(jnp.float32) + 0.1 * (clip * grad)
    kept = 0.95 * second + 0.05 * (clip * clip) * rows / width_total
    return (moved / corr1 / (jnp.sqrt(kept / corr2)[:, None] + 1e-08)).astype(jnp.bfloat16)


def general(token_ids, hidden, embed_cot, logit_cot, emb_first, emb_second, head_first, head_second, step):
    row_count, columns = emb_first.shape
    tok_count = hidden.shape[0]
    owner_count = lax.axis_size("vocab")
    width_total = columns * lax.axis_size("width")
    own_index = lax.axis_index("vocab")
    head_grad = lax.dot_general(
        lax.all_gather(logit_cot, "width", axis=0, tiled=True),
        lax.all_gather(hidden, "vocab", axis=0, tiled=True),
        (((0,), (0,)), ((), ())),
        preferred_element_type=jnp.float32,
    )
    slot_count = (tok_count + owner_count - 1) // owner_count + 1
    own_ids = lax.dynamic_slice_in_dim(token_ids, own_index * tok_count, tok_count, 0)
    dest_owner = own_ids // row_count
    chosen = (dest_owner[:, None] == jnp.arange(owner_count, dtype=jnp.int32)[None, :]).astype(jnp.int32)
    order_in = jnp.sum(jnp.cumsum(chosen, axis=0) * chosen, axis=1) - 1
    target_slot = dest_owner * slot_count + order_in
    outbox = jnp.zeros((owner_count * slot_count, columns), jnp.bfloat16).at[target_slot].set(embed_cot)
    arrived = lax.all_to_all(outbox, "vocab", split_axis=0, concat_axis=0, tiled=True)
    all_blocks = token_ids.reshape(owner_count, tok_count) - own_index * row_count
    ours = ((all_blocks >= 0) & (all_blocks < row_count)).astype(jnp.int32)
    slot_index = jnp.arange(owner_count, dtype=jnp.int32)[:, None] * slot_count + jnp.cumsum(ours, axis=1) - 1
    slot_index = jnp.where(ours > 0, slot_index, owner_count * slot_count)
    slot_row = jnp.full((owner_count * slot_count,), row_count, jnp.int32)
    slot_row = slot_row.at[slot_index.reshape(-1)].set(all_blocks.reshape(-1), mode="drop")
    emb_grad = jnp.zeros((row_count, columns), jnp.float32).at[slot_row].add(arrived.astype(jnp.float32), mode="drop")
    emb_rows, head_rows = lax.psum(
        (jnp.sum(emb_grad * emb_grad, axis=1), jnp.sum(head_grad * head_grad, axis=1)), "width"
    )
    total = lax.psum(jnp.sum(emb_rows) + jnp.sum(head_rows), "vocab")
    clip = 1.0 / (jnp.sqrt(total) + 1e-06)
    count = step[0].astype(jnp.float32)
    corr1 = 1.0 - jnp.power(jnp.float32(0.9), count)
    corr2 = 1.0 - jnp.power(jnp.float32(0.95), count)
    return (
        adam_rows(emb_grad, emb_rows, emb_first, emb_second, clip, corr1, corr2, width_total),
        adam_rows(head_grad, head_rows, head_first, head_second, clip, corr1, corr2, width_total),
    )


def solution(mesh):
    owners, groups = mesh.shape["vocab"], mesh.shape["width"]
    paired_up = groups == 4 and owners == 2 * groups
    placed = (
        P(),
        P("vocab", "width"),
        P("vocab", "width"),
        P("width", "vocab"),
        P("vocab", "width"),
        P("vocab"),
        P("vocab", "width"),
        P("vocab"),
        P(),
    )
    return jax.shard_map(
        paired if paired_up else general,
        mesh=mesh,
        in_specs=placed,
        out_specs=(P("vocab", "width"), P("vocab", "width")),
        check_vma=False,
    )
```

```python
import functools

import jax
import jax.numpy as jnp
from jax import lax
from jax.experimental import pallas as pl
from jax.experimental.pallas import tpu as pltpu
from jax.sharding import PartitionSpec as P


LANES = 128


def round_up(value, multiple):
    return (value + multiple - 1) // multiple * multiple


def swap(x, axis, distance):
    return lax.ppermute(x, axis, [(i, i ^ distance) for i in range(lax.axis_size(axis))])


def row_sums(squares, spare):
    spare[...] = jnp.zeros_like(spare)
    spare[: squares.shape[0], :] = squares
    return jnp.sum(spare[...].T, axis=0, keepdims=True)


def fold(square):
    total = square[:, :LANES]
    for start in range(LANES, square.shape[1], LANES):
        total = total + square[:, start : start + LANES]
    return total


def pack_kernel(rows, groups, slot_count, ids_ref, cot_hbm, near_ref, far_ref, slot_row_ref, cot_ref, sem):
    fetch = pltpu.make_async_copy(cot_hbm, cot_ref, sem)
    fetch.start()
    owners, tok = ids_ref.shape
    slots = owners * slot_count
    index = lax.axis_index("vocab")
    owner = lax.broadcasted_iota(jnp.int32, (owners, tok), 0)
    relative = owner ^ index
    before = lax.broadcasted_iota(jnp.int32, (tok, tok), 0) < lax.broadcasted_iota(jnp.int32, (tok, tok), 1)
    before = before.astype(jnp.float32).astype(jnp.bfloat16)

    def order_of(member):
        return jnp.dot(member.astype(jnp.float32).astype(jnp.bfloat16), before, preferred_element_type=jnp.float32)

    own = ids_ref[pl.ds(index, 1), :]
    to_owner = (own >= owner * rows) & (own < owner * rows + rows)
    first_slot = ((relative & 1) * groups + (relative >> 1)) * slot_count
    slot = jnp.sum(jnp.where(to_owner, first_slot.astype(jnp.float32) + order_of(to_owner), 0.0), axis=0, keepdims=True)
    wanted = lax.broadcasted_iota(jnp.int32, (slots, tok), 0).astype(jnp.float32)
    chosen = (wanted == slot).astype(jnp.float32).astype(jnp.bfloat16)
    half = slots // 2
    fetch.wait()
    near_ref[...] = jnp.dot(chosen[:half], cot_ref[...], preferred_element_type=jnp.float32).astype(jnp.bfloat16)
    far_ref[...] = jnp.dot(chosen[half:], cot_ref[...], preferred_element_type=jnp.float32).astype(jnp.bfloat16)

    local = ids_ref[...] - index * rows
    ours = (local >= 0) & (local < rows)
    slot = jnp.where(ours, (relative * slot_count).astype(jnp.float32) + order_of(ours), -1.0)
    local = local.astype(jnp.float32) + 1.0
    row = jnp.zeros((slots, 1), jnp.float32)
    for source in range(owners):
        hit = wanted == slot[source : source + 1, :]
        row = row + jnp.sum(jnp.where(hit, local[source : source + 1, :], 0.0), axis=1, keepdims=True)
    slot_row_ref[...] = jnp.broadcast_to(row - 1.0, (slots, LANES)).T[0:1, :]


def merge_kernel(groups, slot_count, near_ref, far_ref, *pair_refs):
    for k in range(groups):
        at = slice(k * slot_count, (k + 1) * slot_count)
        pair_refs[k][:slot_count, :] = near_ref[at, :]
        pair_refs[k][slot_count:, :] = far_ref[at, :]


def partial_kernel(groups, tok, depth, step_cols, *refs):
    early = 2 * (groups - 1)
    hid, logit = refs[:early], refs[early : early + groups]
    grad_ref, left_ref, last_ref, right_ref = refs[early + groups : early + groups + 4]
    logit_buf, own_ref, left_buf, sems = refs[early + groups + 4 :]
    own_tokens = pltpu.make_async_copy(hid[0], own_ref, sems.at[0])
    own_logits = pltpu.make_async_copy(logit[0], logit_buf.at[0], sems.at[1])
    own_tokens.start()
    own_logits.start()
    index, column_index = lax.axis_index("vocab"), lax.axis_index("width")
    is_low = (index & 1) == 0
    first_group = (index >> 1) ^ column_index
    for j in range(1, groups):
        logit_buf[j] = logit[j][...]
    left_buf[...] = jnp.zeros_like(left_buf)
    right_ref[...] = jnp.zeros_like(right_ref)
    for at in range(1, early):
        right_ref[at * depth : at * depth + tok, :] = hid[at][...]
    own_tokens.wait()
    right_ref[:tok, :] = own_ref[...]
    own_logits.wait()
    for k in range(groups):
        block = logit_buf[first_group ^ k]
        low, high = block[:tok, :], block[tok:, :]
        left_buf[2 * k * depth : 2 * k * depth + tok, :] = jnp.where(is_low, low, high)
        left_buf[(2 * k + 1) * depth : (2 * k + 1) * depth + tok, :] = jnp.where(is_low, high, low)
    left_ref[...] = left_buf[: early * depth, :].T
    last_ref[...] = left_buf[early * depth :, :].T
    for start in range(0, grad_ref.shape[1], step_cols):
        cols = slice(start, start + step_cols)
        grad_ref[:, cols] = jnp.dot(left_ref[...], right_ref[:, cols], preferred_element_type=jnp.float32)


def embed_kernel(groups, step_cols, slot_row_ref, *refs):
    pairs = refs[:groups]
    rows_ref, pick_ref, emb_ref, spare = refs[groups:]
    rows, slots = pick_ref.shape
    each = slots // groups
    for k in range(groups):
        emb_ref[k * each : (k + 1) * each, :] = pairs[k][...]
    row_of = lax.broadcasted_iota(jnp.int32, (rows, slots), 0).astype(jnp.float32)
    pick_ref[...] = (row_of == slot_row_ref[...]).astype(jnp.float32).astype(jnp.bfloat16)
    squares = jnp.zeros((rows, LANES), jnp.float32)
    for start in range(0, emb_ref.shape[1], step_cols):
        cols = slice(start, start + step_cols)
        grad = jnp.dot(pick_ref[...], emb_ref[:, cols], preferred_element_type=jnp.float32)
        squares = squares + fold(grad * grad)
    rows_ref[...] = row_sums(squares, spare)


def norms_kernel(tok, depth, step_cols, near_ref, far_ref, last_ref, part_ref, emb_rows_ref, stats_ref, totals_ref, right_ref, spare):
    right_ref[...] = jnp.zeros_like(right_ref)
    right_ref[:tok, :] = near_ref[...]
    right_ref[depth : depth + tok, :] = far_ref[...]
    rows, columns = part_ref.shape
    squares = jnp.zeros((rows, LANES), jnp.float32)
    for start in range(0, columns, step_cols):
        cols = slice(start, start + step_cols)
        grad = part_ref[:, cols] + jnp.dot(last_ref[...], right_ref[:, cols], preferred_element_type=jnp.float32)
        squares = squares + fold(grad * grad)
    head_rows = row_sums(squares, spare)
    emb_rows = emb_rows_ref[...]
    total = jnp.sum(head_rows + emb_rows, axis=1, keepdims=True)
    stats_ref[...] = jnp.zeros_like(stats_ref)
    stats_ref[0:1, :] = head_rows
    stats_ref[1:2, :] = emb_rows
    totals_ref[...] = jnp.broadcast_to(total, totals_ref.shape)


def update_kernel(width_total, width, scalar_ref, stats_ref, total_ref, second_ref, left_ref, last_ref, right_ref, right_last_ref,
                  pick_ref, emb_ref, emb_first_hbm, head_first_hbm, emb_hbm, head_hbm,
                  emb_first, head_first, emb_out, head_out, *rest):
    grads, (keep_scale, grad_scale, in_sems, out_sems) = rest[:4], rest[4:]
    rows, columns = emb_out.shape
    steps = columns // width
    ahead = min(2, steps)

    def chunk(step):
        return slice(step * width, (step + 1) * width)

    def move(step, table, out):
        cols = chunk(step)
        if out:
            near, far = ((head_out, head_hbm), (emb_out, emb_hbm))[table]
            return pltpu.make_async_copy(near.at[:, cols], far.at[:, cols], out_sems.at[step, table])
        near, far = ((head_first, head_first_hbm), (emb_first, emb_first_hbm))[table]
        return pltpu.make_async_copy(far.at[:, cols], near.at[:, cols], in_sems.at[step, table])

    def multiply(step):
        cols, into = chunk(step), grads[2 * (step % 2) : 2 * (step % 2) + 2]
        left = jnp.concatenate([left_ref[...], last_ref[...]], axis=1)
        right = jnp.concatenate([right_ref[:, cols], right_last_ref[:, cols]], axis=0)
        into[0][...] = jnp.dot(left, right, preferred_element_type=jnp.float32)
        into[1][...] = jnp.dot(pick_ref[...], emb_ref[:, cols], preferred_element_type=jnp.float32)

    for step in range(ahead):
        for table in range(2):
            move(step, table, False).start()
    multiply(0)
    total = jnp.sum(total_ref[...], axis=0, keepdims=True)
    clip = 1.0 / (jnp.sqrt(total[:, 0:1]) + 1e-06)
    corr1, corr2 = scalar_ref[0], scalar_ref[1]
    for at in range(2):
        kept = 0.95 * second_ref[at : at + 1, :] + 0.05 * (clip * clip) * stats_ref[at : at + 1, :] / width_total
        inverse = 1.0 / (corr1 * (jnp.sqrt(kept / corr2) + 1e-08))
        by_row = jnp.broadcast_to(inverse, (LANES, inverse.shape[1])).T
        keep_scale[at] = 0.9 * by_row
        grad_scale[at] = (0.1 * clip) * by_row

    for step in range(steps):
        for table in range(2):
            move(step, table, False).wait()
            if step + ahead < steps:
                move(step + ahead, table, False).start()
        if step + 1 < steps:
            multiply(step + 1)
        for table, (first, out) in enumerate(((head_first, head_out), (emb_first, emb_out))):
            grad = grads[2 * (step % 2) + table]
            for row in range(0, rows, 8):
                here = slice(row, min(row + 8, rows))
                kept, scale = keep_scale[table, here, :], grad_scale[table, here, :]
                for start in range(0, width, LANES):
                    to = slice(step * width + start, step * width + start + LANES)
                    moved = kept * first[here, to].astype(jnp.float32) + scale * grad[here, start : start + LANES]
                    out[here, to] = moved.astype(jnp.bfloat16)
            move(step, table, True).start()

    for step in range(steps):
        for table in range(2):
            move(step, table, True).wait()


def whole():
    return pl.BlockSpec(memory_space=pltpu.VMEM)


def keep(array):
    return pltpu.with_memory_space_constraint(array, pltpu.HBM)


def in_hbm():
    return pl.BlockSpec(memory_space=pltpu.HBM)


def call(kernel, out_shapes, in_specs, scratch, mib, flops, args):
    return pl.pallas_call(
        kernel,
        out_shape=tuple(jax.ShapeDtypeStruct(shape, dtype) for shape, dtype in out_shapes),
        in_specs=in_specs,
        out_specs=tuple(whole() for _ in out_shapes),
        scratch_shapes=scratch,
        compiler_params=pltpu.CompilerParams(vmem_limit_bytes=mib * 1024 * 1024),
        cost_estimate=pl.CostEstimate(flops=flops, bytes_accessed=1024, transcendentals=0),
    )(*args)


def paired(*arrays):
    return paired_body(*arrays)


def paired_body(token_ids, hidden, embed_cot, logit_cot, emb_first, emb_second, head_first, head_second, step):
    rows, columns = emb_first.shape
    tok = hidden.shape[0]
    owners, groups = lax.axis_size("vocab"), lax.axis_size("width")
    width_total = columns * groups
    slot_count = (tok + owners - 1) // owners + 1
    slots = owners * slot_count
    depth = round_up(tok, 64)
    lanes = round_up(rows, LANES)
    bf16, f32 = jnp.bfloat16, jnp.float32

    hid = [hidden] + [None] * (2 * groups - 1)
    logit = [logit_cot] + [None] * (groups - 1)
    logit[1] = swap(logit_cot, "width", 1)
    hid[1] = swap(hidden, "vocab", 1)
    for k in range(1, groups):
        low = k & -k
        hid[2 * k] = swap(hid[2 * (k - low)], "vocab", 2 * low)
    near, far, slot_row = call(
        functools.partial(pack_kernel, rows, groups, slot_count),
        (((slots // 2, columns), bf16), ((slots // 2, columns), bf16), ((1, slots), f32)),
        [whole(), in_hbm()], [pltpu.VMEM((tok, columns), bf16), pltpu.SemaphoreType.DMA], 8, 1000000,
        (token_ids.reshape(owners, tok), keep(embed_cot)),
    )
    across = swap(far, "vocab", 1)
    for j in range(2, groups):
        logit[j] = swap(logit[j - 1], "width", 1) if j & 1 else swap(logit_cot, "width", j)
    emb = list(call(
        functools.partial(merge_kernel, groups, slot_count),
        (((2 * slot_count, columns), bf16),) * groups, [whole()] * 2, [], 8, 1000000, (near, across),
    ))
    for k in range(1, groups):
        hid[2 * k + 1] = swap(hid[2 * k], "vocab", 1)
        emb[k] = swap(emb[k], "vocab", 2 * k)

    early = 2 * (groups - 1)
    part, left, last, right = call(
        functools.partial(partial_kernel, groups, tok, depth, 512),
        (((rows, columns), f32), ((rows, early * depth), bf16), ((rows, 2 * depth), bf16), ((early * depth, columns), bf16)),
        [in_hbm()] + [whole()] * (early - 1) + [in_hbm()] + [whole()] * (groups - 1),
        [
            pltpu.VMEM((groups,) + logit_cot.shape, bf16),
            pltpu.VMEM((tok, columns), bf16),
            pltpu.VMEM((2 * groups * depth, rows), bf16),
            pltpu.SemaphoreType.DMA((2,)),
        ],
        24, 1000000000, (keep(hidden), *hid[1:early], keep(logit_cot), *logit[1:]),
    )
    emb_rows, pick, emb_all = call(
        functools.partial(embed_kernel, groups, 512),
        (((1, lanes), f32), ((rows, slots), bf16), ((slots, columns), bf16)), [whole()] * (1 + groups),
        [pltpu.VMEM((lanes, LANES), f32)], 16, 100000000, (slot_row, *emb),
    )
    stats, totals, right_last = call(
        functools.partial(norms_kernel, tok, depth, 512),
        (((4, lanes), f32), ((owners * groups, LANES), f32), ((2 * depth, columns), bf16)),
        [whole()] * 5, [pltpu.VMEM((lanes, LANES), f32)], 24, 300000000,
        (hid[early], hid[early + 1], last, part, emb_rows),
    )

    distance = 1
    while distance < groups:
        stats = stats + swap(stats, "width", distance)
        distance *= 2
    total = lax.all_to_all(totals, ("vocab", "width"), 0, 0, tiled=True)

    count = step[0].astype(f32)
    corr1 = 1.0 - jnp.power(f32(0.9), count)
    corr2 = 1.0 - jnp.power(f32(0.95), count)
    second = jnp.pad(jnp.stack([head_second, emb_second]), ((0, 0), (0, lanes - rows)), constant_values=1.0)
    step_cols = min(columns, 512)
    steps = columns // step_cols
    return pl.pallas_call(
        functools.partial(update_kernel, float(width_total), step_cols),
        out_shape=(jax.ShapeDtypeStruct((rows, columns), bf16),) * 2,
        in_specs=[pl.BlockSpec(memory_space=pltpu.SMEM)] + [whole()] * 9 + [in_hbm()] * 2,
        out_specs=(in_hbm(), in_hbm()),
        scratch_shapes=[pltpu.VMEM((rows, columns), bf16)] * 4
        + [pltpu.VMEM((rows, step_cols), f32)] * 4
        + [pltpu.VMEM((2, lanes, LANES), f32)] * 2
        + [pltpu.SemaphoreType.DMA((steps, 2))] * 2,
        compiler_params=pltpu.CompilerParams(vmem_limit_bytes=32 * 1024 * 1024),
        name="update",
    )(
        jnp.stack([corr1, corr2]), stats, total, second, left, last, right, right_last, pick, emb_all,
        keep(emb_first), keep(head_first),
    )


def adam_rows(grad, rows, first, second, clip, corr1, corr2, width_total):
    moved = 0.9 * first.astype(jnp.float32) + 0.1 * (clip * grad)
    kept = 0.95 * second + 0.05 * (clip * clip) * rows / width_total
    return (moved / corr1 / (jnp.sqrt(kept / corr2)[:, None] + 1e-08)).astype(jnp.bfloat16)


def general(token_ids, hidden, embed_cot, logit_cot, emb_first, emb_second, head_first, head_second, step):
    row_count, columns = emb_first.shape
    tok_count = hidden.shape[0]
    owner_count = lax.axis_size("vocab")
    width_total = columns * lax.axis_size("width")
    own_index = lax.axis_index("vocab")
    head_grad = lax.dot_general(
        lax.all_gather(logit_cot, "width", axis=0, tiled=True),
        lax.all_gather(hidden, "vocab", axis=0, tiled=True),
        (((0,), (0,)), ((), ())),
        preferred_element_type=jnp.float32,
    )
    slot_count = (tok_count + owner_count - 1) // owner_count + 1
    own_ids = lax.dynamic_slice_in_dim(token_ids, own_index * tok_count, tok_count, 0)
    dest_owner = own_ids // row_count
    chosen = (dest_owner[:, None] == jnp.arange(owner_count, dtype=jnp.int32)[None, :]).astype(jnp.int32)
    order_in = jnp.sum(jnp.cumsum(chosen, axis=0) * chosen, axis=1) - 1
    target_slot = dest_owner * slot_count + order_in
    outbox = jnp.zeros((owner_count * slot_count, columns), jnp.bfloat16).at[target_slot].set(embed_cot)
    arrived = lax.all_to_all(outbox, "vocab", split_axis=0, concat_axis=0, tiled=True)
    all_blocks = token_ids.reshape(owner_count, tok_count) - own_index * row_count
    ours = ((all_blocks >= 0) & (all_blocks < row_count)).astype(jnp.int32)
    slot_index = jnp.arange(owner_count, dtype=jnp.int32)[:, None] * slot_count + jnp.cumsum(ours, axis=1) - 1
    slot_index = jnp.where(ours > 0, slot_index, owner_count * slot_count)
    slot_row = jnp.full((owner_count * slot_count,), row_count, jnp.int32)
    slot_row = slot_row.at[slot_index.reshape(-1)].set(all_blocks.reshape(-1), mode="drop")
    emb_grad = jnp.zeros((row_count, columns), jnp.float32).at[slot_row].add(arrived.astype(jnp.float32), mode="drop")
    emb_rows, head_rows = lax.psum(
        (jnp.sum(emb_grad * emb_grad, axis=1), jnp.sum(head_grad * head_grad, axis=1)), "width"
    )
    total = lax.psum(jnp.sum(emb_rows) + jnp.sum(head_rows), "vocab")
    clip = 1.0 / (jnp.sqrt(total) + 1e-06)
    count = step[0].astype(jnp.float32)
    corr1 = 1.0 - jnp.power(jnp.float32(0.9), count)
    corr2 = 1.0 - jnp.power(jnp.float32(0.95), count)
    return (
        adam_rows(emb_grad, emb_rows, emb_first, emb_second, clip, corr1, corr2, width_total),
        adam_rows(head_grad, head_rows, head_first, head_second, clip, corr1, corr2, width_total),
    )


def solution(mesh):
    owners, groups = mesh.shape["vocab"], mesh.shape["width"]
    paired_up = groups == 4 and owners == 2 * groups
    placed = (
        P(),
        P("vocab", "width"),
        P("vocab", "width"),
        P("width", "vocab"),
        P("vocab", "width"),
        P("vocab"),
        P("vocab", "width"),
        P("vocab"),
        P(),
    )
    return jax.shard_map(
        paired if paired_up else general,
        mesh=mesh,
        in_specs=placed,
        out_specs=(P("vocab", "width"), P("vocab", "width")),
        check_vma=False,
    )
```

```python
import functools

import jax
import jax.numpy as jnp
from jax import lax
from jax.experimental import pallas as pl
from jax.experimental.pallas import tpu as pltpu
from jax.sharding import PartitionSpec as P


LANES = 128


def round_up(value, multiple):
    return (value + multiple - 1) // multiple * multiple


def swap(x, axis, distance):
    return lax.ppermute(x, axis, [(i, i ^ distance) for i in range(lax.axis_size(axis))])


def row_sums(squares, spare):
    spare[...] = jnp.zeros_like(spare)
    spare[: squares.shape[0], :] = squares
    return jnp.sum(spare[...].T, axis=0, keepdims=True)


def fold(square):
    total = square[:, :LANES]
    for start in range(LANES, square.shape[1], LANES):
        total = total + square[:, start : start + LANES]
    return total


def pack_kernel(rows, groups, slot_count, ids_ref, cot_hbm, near_ref, far_ref, slot_row_ref, cot_ref, sem):
    fetch = pltpu.make_async_copy(cot_hbm, cot_ref, sem)
    fetch.start()
    owners, tok = ids_ref.shape
    slots = owners * slot_count
    index = lax.axis_index("vocab")
    owner = lax.broadcasted_iota(jnp.int32, (owners, tok), 0)
    relative = owner ^ index
    before = lax.broadcasted_iota(jnp.int32, (tok, tok), 0) < lax.broadcasted_iota(jnp.int32, (tok, tok), 1)
    before = before.astype(jnp.float32).astype(jnp.bfloat16)

    def order_of(member):
        return jnp.dot(member.astype(jnp.float32).astype(jnp.bfloat16), before, preferred_element_type=jnp.float32)

    own = ids_ref[pl.ds(index, 1), :]
    to_owner = (own >= owner * rows) & (own < owner * rows + rows)
    first_slot = ((relative & 1) * groups + (relative >> 1)) * slot_count
    slot = jnp.sum(jnp.where(to_owner, first_slot.astype(jnp.float32) + order_of(to_owner), 0.0), axis=0, keepdims=True)
    wanted = lax.broadcasted_iota(jnp.int32, (slots, tok), 0).astype(jnp.float32)
    chosen = (wanted == slot).astype(jnp.float32).astype(jnp.bfloat16)
    half = slots // 2
    fetch.wait()
    near_ref[...] = jnp.dot(chosen[:half], cot_ref[...], preferred_element_type=jnp.float32).astype(jnp.bfloat16)
    far_ref[...] = jnp.dot(chosen[half:], cot_ref[...], preferred_element_type=jnp.float32).astype(jnp.bfloat16)

    local = ids_ref[...] - index * rows
    ours = (local >= 0) & (local < rows)
    slot = jnp.where(ours, (relative * slot_count).astype(jnp.float32) + order_of(ours), -1.0)
    local = local.astype(jnp.float32) + 1.0
    row = jnp.zeros((slots, 1), jnp.float32)
    for source in range(owners):
        hit = wanted == slot[source : source + 1, :]
        row = row + jnp.sum(jnp.where(hit, local[source : source + 1, :], 0.0), axis=1, keepdims=True)
    slot_row_ref[...] = jnp.broadcast_to(row - 1.0, (slots, LANES)).T[0:1, :]


def merge_kernel(groups, slot_count, near_ref, far_ref, *pair_refs):
    for k in range(groups):
        at = slice(k * slot_count, (k + 1) * slot_count)
        pair_refs[k][:slot_count, :] = near_ref[at, :]
        pair_refs[k][slot_count:, :] = far_ref[at, :]


def partial_kernel(groups, tok, depth, step_cols, *refs):
    early = 2 * (groups - 1)
    hid, logit = refs[:early], refs[early : early + groups]
    grad_ref, left_ref, last_ref, right_ref = refs[early + groups : early + groups + 4]
    logit_buf, own_ref, left_buf, sems = refs[early + groups + 4 :]
    own_tokens = pltpu.make_async_copy(hid[0], own_ref, sems.at[0])
    own_logits = pltpu.make_async_copy(logit[0], logit_buf.at[0], sems.at[1])
    own_tokens.start()
    own_logits.start()
    index, column_index = lax.axis_index("vocab"), lax.axis_index("width")
    is_low = (index & 1) == 0
    first_group = (index >> 1) ^ column_index
    for j in range(1, groups):
        logit_buf[j] = logit[j][...]
    left_buf[...] = jnp.zeros_like(left_buf)
    right_ref[...] = jnp.zeros_like(right_ref)
    for at in range(1, early):
        right_ref[at * depth : at * depth + tok, :] = hid[at][...]
    own_tokens.wait()
    right_ref[:tok, :] = own_ref[...]
    own_logits.wait()
    for k in range(groups):
        block = logit_buf[first_group ^ k]
        low, high = block[:tok, :], block[tok:, :]
        left_buf[2 * k * depth : 2 * k * depth + tok, :] = jnp.where(is_low, low, high)
        left_buf[(2 * k + 1) * depth : (2 * k + 1) * depth + tok, :] = jnp.where(is_low, high, low)
    left_ref[...] = left_buf[: early * depth, :].T
    last_ref[...] = left_buf[early * depth :, :].T
    for start in range(0, grad_ref.shape[1], step_cols):
        cols = slice(start, start + step_cols)
        grad_ref[:, cols] = jnp.dot(left_ref[...], right_ref[:, cols], preferred_element_type=jnp.float32)


def embed_kernel(groups, step_cols, slot_row_ref, *refs):
    pairs = refs[:groups]
    rows_ref, pick_ref, emb_ref, spare = refs[groups:]
    rows, slots = pick_ref.shape
    each = slots // groups
    for k in range(groups):
        emb_ref[k * each : (k + 1) * each, :] = pairs[k][...]
    row_of = lax.broadcasted_iota(jnp.int32, (rows, slots), 0).astype(jnp.float32)
    pick_ref[...] = (row_of == slot_row_ref[...]).astype(jnp.float32).astype(jnp.bfloat16)
    squares = jnp.zeros((rows, LANES), jnp.float32)
    for start in range(0, emb_ref.shape[1], step_cols):
        cols = slice(start, start + step_cols)
        grad = jnp.dot(pick_ref[...], emb_ref[:, cols], preferred_element_type=jnp.float32)
        squares = squares + fold(grad * grad)
    rows_ref[...] = row_sums(squares, spare)


def norms_kernel(tok, depth, step_cols, near_ref, far_ref, last_ref, part_ref, emb_rows_ref, stats_ref, totals_ref, right_ref, spare):
    right_ref[...] = jnp.zeros_like(right_ref)
    right_ref[:tok, :] = near_ref[...]
    right_ref[depth : depth + tok, :] = far_ref[...]
    rows, columns = part_ref.shape
    squares = jnp.zeros((rows, LANES), jnp.float32)
    for start in range(0, columns, step_cols):
        cols = slice(start, start + step_cols)
        grad = part_ref[:, cols] + jnp.dot(last_ref[...], right_ref[:, cols], preferred_element_type=jnp.float32)
        squares = squares + fold(grad * grad)
    head_rows = row_sums(squares, spare)
    emb_rows = emb_rows_ref[...]
    total = jnp.sum(head_rows + emb_rows, axis=1, keepdims=True)
    stats_ref[...] = jnp.zeros_like(stats_ref)
    stats_ref[0:1, :] = head_rows
    stats_ref[1:2, :] = emb_rows
    totals_ref[...] = jnp.broadcast_to(total, totals_ref.shape)


def update_kernel(width_total, width, scalar_ref, stats_ref, total_ref, second_ref, left_ref, last_ref, right_ref, right_last_ref,
                  pick_ref, emb_ref, emb_first_hbm, head_first_hbm, emb_hbm, head_hbm,
                  emb_first, head_first, emb_out, head_out, *rest):
    grads, (keep_scale, grad_scale, in_sems, out_sems) = rest[:4], rest[4:]
    rows, columns = emb_out.shape
    steps = columns // width
    ahead = min(4, steps)

    def chunk(step):
        return slice(step * width, (step + 1) * width)

    def move(step, table, out):
        cols = chunk(step)
        if out:
            near, far = ((head_out, head_hbm), (emb_out, emb_hbm))[table]
            return pltpu.make_async_copy(near.at[:, cols], far.at[:, cols], out_sems.at[step, table])
        near, far = ((head_first, head_first_hbm), (emb_first, emb_first_hbm))[table]
        return pltpu.make_async_copy(far.at[:, cols], near.at[:, cols], in_sems.at[step, table])

    def multiply(step, piece):
        into = grads[2 * (step % 2) : 2 * (step % 2) + 2]
        if piece == 2:
            into[1][...] = jnp.dot(pick_ref[...], emb_ref[:, chunk(step)], preferred_element_type=jnp.float32)
            return
        half = width // 2
        cols = slice(step * width + piece * half, step * width + (piece + 1) * half)
        left = jnp.concatenate([left_ref[...], last_ref[...]], axis=1)
        right = jnp.concatenate([right_ref[:, cols], right_last_ref[:, cols]], axis=0)
        into[0][:, piece * half : (piece + 1) * half] = jnp.dot(left, right, preferred_element_type=jnp.float32)

    def combine(step, rows_here):
        for table, (first, out) in enumerate(((head_first, head_out), (emb_first, emb_out))):
            grad = grads[2 * (step % 2) + table]
            for row in range(rows_here.start, rows_here.stop, 8):
                here = slice(row, min(row + 8, rows_here.stop))
                kept, scale = keep_scale[table, here, :], grad_scale[table, here, :]
                for start in range(0, width, LANES):
                    to = slice(step * width + start, step * width + start + LANES)
                    moved = kept * first[here, to].astype(jnp.float32) + scale * grad[here, start : start + LANES]
                    out[here, to] = moved.astype(jnp.bfloat16)

    for step in range(ahead):
        for table in range(2):
            move(step, table, False).start()
    for piece in range(3):
        multiply(0, piece)
    total = jnp.sum(total_ref[...], axis=0, keepdims=True)
    clip = 1.0 / (jnp.sqrt(total[:, 0:1]) + 1e-06)
    corr1, corr2 = scalar_ref[0], scalar_ref[1]
    for at in range(2):
        kept = 0.95 * second_ref[at : at + 1, :] + 0.05 * (clip * clip) * stats_ref[at : at + 1, :] / width_total
        inverse = 1.0 / (corr1 * (jnp.sqrt(kept / corr2) + 1e-08))
        by_row = jnp.broadcast_to(inverse, (LANES, inverse.shape[1])).T
        keep_scale[at] = 0.9 * by_row
        grad_scale[at] = (0.1 * clip) * by_row

    for step in range(steps):
        for table in range(2):
            move(step, table, False).wait()
            if step + ahead < steps:
                move(step + ahead, table, False).start()
        edges = [0] + [rows * piece // 24 * 8 for piece in (1, 2)] + [rows]
        for piece in range(3):

            @pl.when(corr1 > 0.0)
            def _():
                if step + 1 < steps:
                    multiply(step + 1, piece)
                combine(step, slice(edges[piece], edges[piece + 1]))

        for table in range(2):
            move(step, table, True).start()

    for step in range(steps):
        for table in range(2):
            move(step, table, True).wait()


def whole():
    return pl.BlockSpec(memory_space=pltpu.VMEM)


def keep(array):
    return pltpu.with_memory_space_constraint(array, pltpu.HBM)


def in_hbm():
    return pl.BlockSpec(memory_space=pltpu.HBM)


def call(kernel, out_shapes, in_specs, scratch, mib, flops, args):
    return pl.pallas_call(
        kernel,
        out_shape=tuple(jax.ShapeDtypeStruct(shape, dtype) for shape, dtype in out_shapes),
        in_specs=in_specs,
        out_specs=tuple(whole() for _ in out_shapes),
        scratch_shapes=scratch,
        compiler_params=pltpu.CompilerParams(vmem_limit_bytes=mib * 1024 * 1024),
        cost_estimate=pl.CostEstimate(flops=flops, bytes_accessed=1024, transcendentals=0),
    )(*args)


def paired(*arrays):
    return paired_body(*arrays)


def paired_body(token_ids, hidden, embed_cot, logit_cot, emb_first, emb_second, head_first, head_second, step):
    rows, columns = emb_first.shape
    tok = hidden.shape[0]
    owners, groups = lax.axis_size("vocab"), lax.axis_size("width")
    width_total = columns * groups
    slot_count = (tok + owners - 1) // owners + 1
    slots = owners * slot_count
    depth = round_up(tok, 64)
    lanes = round_up(rows, LANES)
    bf16, f32 = jnp.bfloat16, jnp.float32

    hid = [hidden] + [None] * (2 * groups - 1)
    logit = [logit_cot] + [None] * (groups - 1)
    logit[1] = swap(logit_cot, "width", 1)
    hid[1] = swap(hidden, "vocab", 1)
    for k in range(1, groups):
        low = k & -k
        hid[2 * k] = swap(hid[2 * (k - low)], "vocab", 2 * low)
    near, far, slot_row = call(
        functools.partial(pack_kernel, rows, groups, slot_count),
        (((slots // 2, columns), bf16), ((slots // 2, columns), bf16), ((1, slots), f32)),
        [whole(), in_hbm()], [pltpu.VMEM((tok, columns), bf16), pltpu.SemaphoreType.DMA], 8, 1000000,
        (token_ids.reshape(owners, tok), keep(embed_cot)),
    )
    across = swap(far, "vocab", 1)
    for j in range(2, groups):
        logit[j] = swap(logit[j - 1], "width", 1) if j & 1 else swap(logit_cot, "width", j)
    emb = list(call(
        functools.partial(merge_kernel, groups, slot_count),
        (((2 * slot_count, columns), bf16),) * groups, [whole()] * 2, [], 8, 1000000, (near, across),
    ))
    for k in range(1, groups):
        hid[2 * k + 1] = swap(hid[2 * k], "vocab", 1)
        emb[k] = swap(emb[k], "vocab", 2 * k)

    early = 2 * (groups - 1)
    part, left, last, right = call(
        functools.partial(partial_kernel, groups, tok, depth, 512),
        (((rows, columns), f32), ((rows, early * depth), bf16), ((rows, 2 * depth), bf16), ((early * depth, columns), bf16)),
        [in_hbm()] + [whole()] * (early - 1) + [in_hbm()] + [whole()] * (groups - 1),
        [
            pltpu.VMEM((groups,) + logit_cot.shape, bf16),
            pltpu.VMEM((tok, columns), bf16),
            pltpu.VMEM((2 * groups * depth, rows), bf16),
            pltpu.SemaphoreType.DMA((2,)),
        ],
        24, 1000000000, (keep(hidden), *hid[1:early], keep(logit_cot), *logit[1:]),
    )
    emb_rows, pick, emb_all = call(
        functools.partial(embed_kernel, groups, 512),
        (((1, lanes), f32), ((rows, slots), bf16), ((slots, columns), bf16)), [whole()] * (1 + groups),
        [pltpu.VMEM((lanes, LANES), f32)], 16, 100000000, (slot_row, *emb),
    )
    stats, totals, right_last = call(
        functools.partial(norms_kernel, tok, depth, 512),
        (((4, lanes), f32), ((owners * groups, LANES), f32), ((2 * depth, columns), bf16)),
        [whole()] * 5, [pltpu.VMEM((lanes, LANES), f32)], 24, 300000000,
        (hid[early], hid[early + 1], last, part, emb_rows),
    )

    distance = 1
    while distance < groups:
        stats = stats + swap(stats, "width", distance)
        distance *= 2
    total = lax.all_to_all(totals, ("vocab", "width"), 0, 0, tiled=True)

    count = step[0].astype(f32)
    corr1 = 1.0 - jnp.power(f32(0.9), count)
    corr2 = 1.0 - jnp.power(f32(0.95), count)
    second = jnp.pad(jnp.stack([head_second, emb_second]), ((0, 0), (0, lanes - rows)), constant_values=1.0)
    step_cols = min(columns, 512)
    steps = columns // step_cols
    return pl.pallas_call(
        functools.partial(update_kernel, float(width_total), step_cols),
        out_shape=(jax.ShapeDtypeStruct((rows, columns), bf16),) * 2,
        in_specs=[pl.BlockSpec(memory_space=pltpu.SMEM)] + [whole()] * 9 + [in_hbm()] * 2,
        out_specs=(in_hbm(), in_hbm()),
        scratch_shapes=[pltpu.VMEM((rows, columns), bf16)] * 4
        + [pltpu.VMEM((rows, step_cols), f32)] * 4
        + [pltpu.VMEM((2, lanes, LANES), f32)] * 2
        + [pltpu.SemaphoreType.DMA((steps, 2))] * 2,
        compiler_params=pltpu.CompilerParams(vmem_limit_bytes=32 * 1024 * 1024),
        name="update",
    )(
        jnp.stack([corr1, corr2]), stats, total, second, left, last, right, right_last, pick, emb_all,
        keep(emb_first), keep(head_first),
    )


def adam_rows(grad, rows, first, second, clip, corr1, corr2, width_total):
    moved = 0.9 * first.astype(jnp.float32) + 0.1 * (clip * grad)
    kept = 0.95 * second + 0.05 * (clip * clip) * rows / width_total
    return (moved / corr1 / (jnp.sqrt(kept / corr2)[:, None] + 1e-08)).astype(jnp.bfloat16)


def general(token_ids, hidden, embed_cot, logit_cot, emb_first, emb_second, head_first, head_second, step):
    row_count, columns = emb_first.shape
    tok_count = hidden.shape[0]
    owner_count = lax.axis_size("vocab")
    width_total = columns * lax.axis_size("width")
    own_index = lax.axis_index("vocab")
    head_grad = lax.dot_general(
        lax.all_gather(logit_cot, "width", axis=0, tiled=True),
        lax.all_gather(hidden, "vocab", axis=0, tiled=True),
        (((0,), (0,)), ((), ())),
        preferred_element_type=jnp.float32,
    )
    slot_count = (tok_count + owner_count - 1) // owner_count + 1
    own_ids = lax.dynamic_slice_in_dim(token_ids, own_index * tok_count, tok_count, 0)
    dest_owner = own_ids // row_count
    chosen = (dest_owner[:, None] == jnp.arange(owner_count, dtype=jnp.int32)[None, :]).astype(jnp.int32)
    order_in = jnp.sum(jnp.cumsum(chosen, axis=0) * chosen, axis=1) - 1
    target_slot = dest_owner * slot_count + order_in
    outbox = jnp.zeros((owner_count * slot_count, columns), jnp.bfloat16).at[target_slot].set(embed_cot)
    arrived = lax.all_to_all(outbox, "vocab", split_axis=0, concat_axis=0, tiled=True)
    all_blocks = token_ids.reshape(owner_count, tok_count) - own_index * row_count
    ours = ((all_blocks >= 0) & (all_blocks < row_count)).astype(jnp.int32)
    slot_index = jnp.arange(owner_count, dtype=jnp.int32)[:, None] * slot_count + jnp.cumsum(ours, axis=1) - 1
    slot_index = jnp.where(ours > 0, slot_index, owner_count * slot_count)
    slot_row = jnp.full((owner_count * slot_count,), row_count, jnp.int32)
    slot_row = slot_row.at[slot_index.reshape(-1)].set(all_blocks.reshape(-1), mode="drop")
    emb_grad = jnp.zeros((row_count, columns), jnp.float32).at[slot_row].add(arrived.astype(jnp.float32), mode="drop")
    emb_rows, head_rows = lax.psum(
        (jnp.sum(emb_grad * emb_grad, axis=1), jnp.sum(head_grad * head_grad, axis=1)), "width"
    )
    total = lax.psum(jnp.sum(emb_rows) + jnp.sum(head_rows), "vocab")
    clip = 1.0 / (jnp.sqrt(total) + 1e-06)
    count = step[0].astype(jnp.float32)
    corr1 = 1.0 - jnp.power(jnp.float32(0.9), count)
    corr2 = 1.0 - jnp.power(jnp.float32(0.95), count)
    return (
        adam_rows(emb_grad, emb_rows, emb_first, emb_second, clip, corr1, corr2, width_total),
        adam_rows(head_grad, head_rows, head_first, head_second, clip, corr1, corr2, width_total),
    )


def solution(mesh):
    owners, groups = mesh.shape["vocab"], mesh.shape["width"]
    paired_up = groups == 4 and owners == 2 * groups
    placed = (
        P(),
        P("vocab", "width"),
        P("vocab", "width"),
        P("width", "vocab"),
        P("vocab", "width"),
        P("vocab"),
        P("vocab", "width"),
        P("vocab"),
        P(),
    )
    return jax.shard_map(
        paired if paired_up else general,
        mesh=mesh,
        in_specs=placed,
        out_specs=(P("vocab", "width"), P("vocab", "width")),
        check_vma=False,
    )
```
